32 devices in a mesh: batch: 4 (over z), grid: 8 (over y, x, core).
Axes of the slice: x: 2, y: 2, z: 4, core: 2. Of those that a mesh axis runs over, the one named last changes fastest.
Arguments:
- fields: bfloat16 [1024, 512, 512], P(('batch', 'grid')), parts along dimension 0, may hold values from -18 to 18
- norm_gain: float32 [256], replicated, may hold values from 0.5 to 1.5
- norm_shift: float32 [256], replicated, may hold values from -3 to 3
- first_weight: bfloat16 [2, 8, 32, 32], replicated, may hold values from -0.75 to 0.75
- second_weight: bfloat16 [2, 8, 32, 32], replicated, may hold values from -0.75 to 0.75
- first_bias: float32 [2, 256], replicated, may hold values from -2 to 2
Outputs:
- mixed_fields: bfloat16 [1024, 512, 512], P(('batch', 'grid')), parts along dimension 0
The draws below stay inside these ranges and needn't reach their ends.
There are 4 independent parts, one for each index of `batch`. The reference program is written for one: setup_inputs(seed, part) draws one part's arguments, and reference() takes and returns one part's arrays. A program takes and returns all parts, laid end to end along the dimension named above; an argument that names none is the same for every part. Nothing has to cross between parts.
All inputs are finite; a program needn't handle non-finite values.
Results may differ from the reference program's by a relative error of at most 0.0055.
Values may be sent and summed in bfloat16 or wider, within the bound.
A program may use at most 192 MiB of HBM per device.

```python
import math
import jax
import jax.numpy as jnp
from jax import lax

C = 256
BS = 32
H = 512
W = 512
NB = 8


def draw_fields(key, part):
    first_key = jax.random.fold_in(key, 11)
    ramp = jnp.arange(C, dtype=jnp.float32) / (C - 1)
    base = jnp.clip(jax.random.normal(first_key, (C, H, W), jnp.float32), -4.0, 4.0)
    scale = jnp.power(3.0, ramp)
    return (base * scale[:, None, None]).astype(jnp.bfloat16)


def normal_values(key, extent, scale, bound, kind=jnp.bfloat16):
    entries = scale * jax.random.normal(key, extent, jnp.float32)
    return jnp.clip(entries, min=-bound, max=bound).astype(kind)


def setup_inputs(seed: int = 0, part: int = 0) -> dict:
    splits = jax.random.split(jax.random.key(seed), 7)
    part_splits = jax.random.split(jax.random.fold_in(splits[6], part), 7)
    return {
        "fields": draw_fields(jax.random.fold_in(jax.random.fold_in(splits[6], part), 71), part),
        "norm_gain": jnp.clip(1.0 + 0.1 * jax.random.normal(splits[1], (C,), jnp.float32), 0.5, 1.5),
        "norm_shift": normal_values(splits[2], (C,), 0.5, 3.0, jnp.float32),
        "first_weight": normal_values(splits[3], (2, NB, BS, BS), (2 * BS) ** -0.5, 0.75),
        "second_weight": normal_values(splits[4], (2, NB, BS, BS), (2 * BS) ** -0.5, 0.75),
        "first_bias": normal_values(splits[5], (2, C), 0.3, 2.0, jnp.float32),
    }


def tables(rows, cols):
    half = cols // 2
    col_index = jnp.arange(cols, dtype=jnp.int32)
    mode_index = jnp.arange(half, dtype=jnp.int32)
    angle_w = (col_index[:, None] * mode_index[None, :] % cols).astype(jnp.float32) * (2.0 * math.pi / cols)
    scale_w = 1.0 / math.sqrt(cols)
    fwd_w = jnp.concatenate([jnp.cos(angle_w) * scale_w, -jnp.sin(angle_w) * scale_w], axis=1).astype(jnp.bfloat16)
    weight_k = jnp.where(mode_index == 0, 1.0, 2.0).astype(jnp.float32)
    inv_w = jnp.concatenate([(jnp.cos(angle_w) * weight_k[None, :] * scale_w).T, (-jnp.sin(angle_w) * weight_k[None, :] * scale_w).T], axis=0).astype(jnp.bfloat16)
    row_index = jnp.arange(rows, dtype=jnp.int32)
    angle_h = (row_index[:, None] * row_index[None, :] % rows).astype(jnp.float32) * (2.0 * math.pi / rows)
    scale_h = 1.0 / math.sqrt(rows)
    cos_h = (jnp.cos(angle_h) * scale_h).astype(jnp.bfloat16)
    sin_h = (jnp.sin(angle_h) * scale_h).astype(jnp.bfloat16)
    return (fwd_w, inv_w, cos_h, sin_h)

def mult(form, left, right):
    return jnp.einsum(form, left.astype(jnp.float32), right.astype(jnp.float32), precision=lax.Precision.HIGHEST)

def shrink(values):
    return jnp.maximum(values - 0.01, 0.0) + jnp.minimum(values + 0.01, 0.0)

def mix_modes(real_part, imag_part, first_weight, second_weight, first_bias):
    blocks = first_weight.shape[1]
    width = first_weight.shape[2]
    shape = real_part.shape
    real_blk = real_part.reshape(blocks, width, -1)
    imag_blk = imag_part.reshape(blocks, width, -1)
    bias_blk = first_bias.reshape(2, blocks, width, 1)
    hid_re = jax.nn.relu(mult('bio,bim->bom', first_weight[0], real_blk) - mult('bio,bim->bom', first_weight[1], imag_blk) + bias_blk[0]).astype(jnp.bfloat16)
    hid_im = jax.nn.relu(mult('bio,bim->bom', first_weight[0], imag_blk) + mult('bio,bim->bom', first_weight[1], real_blk) + bias_blk[1]).astype(jnp.bfloat16)
    out_re = mult('bio,bim->bom', second_weight[0], hid_re) - mult('bio,bim->bom', second_weight[1], hid_im)
    out_im = mult('bio,bim->bom', second_weight[0], hid_im) + mult('bio,bim->bom', second_weight[1], hid_re)
    return (shrink(out_re).astype(jnp.bfloat16).reshape(shape), shrink(out_im).astype(jnp.bfloat16).reshape(shape))

def reference(fields, norm_gain, norm_shift, first_weight, second_weight, first_bias):
    channels, rows, cols = fields.shape
    half = cols // 2
    fwd_w, inv_w, cos_h, sin_h = tables(rows, cols)
    values = fields.astype(jnp.float32)
    mean = lax.optimization_barrier(jnp.mean(values, axis=0))
    mean_sq = lax.optimization_barrier(jnp.mean(values * values, axis=0))
    var = mean_sq - mean * mean
    normed = ((values - mean) * lax.rsqrt(var + 1e-05) * norm_gain[:, None, None] + norm_shift[:, None, None]).astype(jnp.bfloat16)
    along_w = mult('chw,wk->chk', normed, fwd_w).astype(jnp.bfloat16).reshape(channels, rows, 2, half)
    first_p = mult('kh,chpq->ckpq', cos_h, along_w)
    first_q = mult('kh,chpq->ckpq', sin_h, along_w)
    modes_re = (first_p[:, :, 0] + first_q[:, :, 1]).astype(jnp.bfloat16)
    modes_im = (first_p[:, :, 1] - first_q[:, :, 0]).astype(jnp.bfloat16)
    shr_re, shr_im = mix_modes(modes_re, modes_im, first_weight, second_weight, first_bias)
    shrunk = jnp.stack([shr_re, shr_im], axis=2)
    back_p = mult('kh,ckpq->chpq', cos_h, shrunk)
    back_q = mult('kh,ckpq->chpq', sin_h, shrunk)
    back_re = (back_p[:, :, 0] - back_q[:, :, 1]).astype(jnp.bfloat16)
    back_im = (back_p[:, :, 1] + back_q[:, :, 0]).astype(jnp.bfloat16)
    backed = jnp.concatenate([back_re, back_im], axis=2)
    filtered = mult('chk,kw->chw', backed, inv_w)
    return (values + filtered).astype(jnp.bfloat16)
```

```python
import math

import jax
import jax.numpy as jnp
from jax import lax
from jax.experimental import pallas as pl
from jax.experimental.pallas import tpu as pltpu
from jax.sharding import PartitionSpec as P


def tables(rows, cols):
    half = cols // 2
    col_index = jnp.arange(cols, dtype=jnp.int32)
    mode_index = jnp.arange(half, dtype=jnp.int32)
    angle_w = (col_index[:, None] * mode_index[None, :] % cols).astype(jnp.float32) * (
        2.0 * math.pi / cols
    )
    scale_w = 1.0 / math.sqrt(cols)
    fwd_w = jnp.concatenate(
        [jnp.cos(angle_w) * scale_w, -jnp.sin(angle_w) * scale_w], axis=1
    ).astype(jnp.bfloat16)
    weight_k = jnp.where(mode_index == 0, 1.0, 2.0).astype(jnp.float32)
    inv_w = jnp.concatenate(
        [
            (jnp.cos(angle_w) * weight_k[None, :] * scale_w).T,
            (-jnp.sin(angle_w) * weight_k[None, :] * scale_w).T,
        ],
        axis=0,
    ).astype(jnp.bfloat16)
    row_index = jnp.arange(rows, dtype=jnp.int32)
    angle_h = (row_index[:, None] * row_index[None, :] % rows).astype(jnp.float32) * (
        2.0 * math.pi / rows
    )
    scale_h = 1.0 / math.sqrt(rows)
    cos_h = (jnp.cos(angle_h) * scale_h).astype(jnp.bfloat16)
    sin_h = (jnp.sin(angle_h) * scale_h).astype(jnp.bfloat16)
    return (fwd_w, inv_w, cos_h, sin_h)


def mult(form, left, right):
    return jnp.einsum(form, left, right, preferred_element_type=jnp.float32)


def shrink(values):
    return jnp.maximum(values - 0.01, 0.0) + jnp.minimum(values + 0.01, 0.0)


def mix_modes(real_part, imag_part, first_weight, second_weight, first_bias):
    blocks = first_weight.shape[1]
    width = first_weight.shape[2]
    shape = real_part.shape
    real_blk = real_part.reshape(blocks, width, -1)
    imag_blk = imag_part.reshape(blocks, width, -1)
    bias_blk = first_bias.reshape(2, blocks, width, 1)
    hid_re = jax.nn.relu(
        mult("bio,bim->bom", first_weight[0], real_blk)
        - mult("bio,bim->bom", first_weight[1], imag_blk)
        + bias_blk[0]
    ).astype(jnp.bfloat16)
    hid_im = jax.nn.relu(
        mult("bio,bim->bom", first_weight[0], imag_blk)
        + mult("bio,bim->bom", first_weight[1], real_blk)
        + bias_blk[1]
    ).astype(jnp.bfloat16)
    out_re = mult("bio,bim->bom", second_weight[0], hid_re) - mult(
        "bio,bim->bom", second_weight[1], hid_im
    )
    out_im = mult("bio,bim->bom", second_weight[0], hid_im) + mult(
        "bio,bim->bom", second_weight[1], hid_re
    )
    return (
        shrink(out_re).astype(jnp.bfloat16).reshape(shape),
        shrink(out_im).astype(jnp.bfloat16).reshape(shape),
    )


def per_device(fields, norm_gain, norm_shift, first_weight, second_weight, first_bias):
    local_ch, rows, cols = fields.shape
    half = cols // 2
    groups = lax.axis_size("grid")
    channels = local_ch * groups
    fwd_w, inv_w, cos_h, sin_h = tables(rows, cols)
    values = fields.astype(jnp.float32)
    start = lax.axis_index("grid") * local_ch
    gain_own = lax.dynamic_slice_in_dim(norm_gain, start, local_ch)
    shift_own = lax.dynamic_slice_in_dim(norm_shift, start, local_ch)
    total_sum, total_sq = lax.psum(
        (jnp.sum(values, axis=0), jnp.sum(values * values, axis=0)), "grid"
    )
    mean = total_sum / channels
    var = total_sq / channels - mean * mean
    normed = (
        (values - mean) * lax.rsqrt(var + 1e-05) * gain_own[:, None, None]
        + shift_own[:, None, None]
    ).astype(jnp.bfloat16)
    along_w = (
        mult("chw,wk->chk", normed, fwd_w).astype(jnp.bfloat16).reshape(local_ch, rows, 2, half)
    )
    first_p = mult("kh,chpq->ckpq", cos_h, along_w)
    first_q = mult("kh,chpq->ckpq", sin_h, along_w)
    modes = jnp.stack(
        [
            (first_p[:, :, 0] + first_q[:, :, 1]).astype(jnp.bfloat16),
            (first_p[:, :, 1] - first_q[:, :, 0]).astype(jnp.bfloat16),
        ],
        axis=2,
    )
    spread = lax.all_to_all(modes, "grid", split_axis=1, concat_axis=0, tiled=True)
    shr_re, shr_im = mix_modes(
        spread[:, :, 0], spread[:, :, 1], first_weight, second_weight, first_bias
    )
    gathered = lax.all_to_all(
        jnp.stack([shr_re, shr_im], axis=2), "grid", split_axis=0, concat_axis=1, tiled=True
    )
    back_p = mult("kh,ckpq->chpq", cos_h, gathered)
    back_q = mult("kh,ckpq->chpq", sin_h, gathered)
    back_re = (back_p[:, :, 0] - back_q[:, :, 1]).astype(jnp.bfloat16)
    back_im = (back_p[:, :, 1] + back_q[:, :, 0]).astype(jnp.bfloat16)
    backed = jnp.concatenate([back_re, back_im], axis=2)
    filtered = mult("chk,kw->chw", backed, inv_w)
    return (values + filtered).astype(jnp.bfloat16)

SUB = 8


def half_tables(cos_h, sin_h):
    rows = cos_h.shape[0]
    mid = rows // 2
    low = jnp.concatenate([cos_h[:mid], cos_h[mid : mid + 1], sin_h[1:mid]], axis=0)
    picked = jnp.arange(mid, dtype=jnp.int32)
    swap = (jnp.where(picked == 0, 0, mid - picked)[:, None] == picked[None, :]).astype(
        jnp.bfloat16
    )
    order = lambda t: jnp.concatenate(
        [t[:, :mid], t[:, mid : mid + 1], t[:, mid + 1 :][:, ::-1]], axis=1
    )
    return low, order(low), swap


def spread_weight(weight):
    eye = jnp.eye(SUB, dtype=weight.dtype)
    real = jnp.einsum("bio,st->bosit", weight[0], eye)
    imag = jnp.einsum("bio,st->bosit", weight[1], eye)
    blocks, width = weight.shape[1], weight.shape[2]
    size = width * SUB
    real = real.reshape(blocks, size, size)
    imag = imag.reshape(blocks, size, size)
    return jnp.concatenate(
        [jnp.concatenate([real, -imag], axis=2), jnp.concatenate([imag, real], axis=2)],
        axis=1,
    )


def split_rows(total, sign):
    mid, half = total.shape[0] // 2, total.shape[1] // 2
    p_re, p_im = total[:mid, :half], total[:mid, half:]
    q_re, q_im = total[mid:, :half], total[mid:, half:]
    edge = lax.broadcasted_iota(jnp.int32, (mid, half), 0) == 0
    t_re = jnp.where(edge, 0.0, q_re)
    t_im = jnp.where(edge, 0.0, q_im)
    if sign < 0:
        t_re, t_im = -t_re, -t_im
    plus = (p_re + t_im, p_im - t_re)
    minus = (
        jnp.where(edge, q_re, p_re - t_im),
        jnp.where(edge, q_im, p_im + t_re),
    )
    return plus, minus


def forward_kernel(x_ref, mean_ref, rstd_ref, gain_ref, shift_ref, fw_ref, fh_ref, out_ref):
    count, rows, cols = x_ref.shape
    mid, half = rows // 2, cols // 2
    step = pl.program_id(0)
    for n in range(count):
        gain = gain_ref[step * count + n]
        shift = shift_ref[step * count + n]
        values = x_ref[n].astype(jnp.float32)
        normed = ((values - mean_ref[...]) * rstd_ref[...] * gain + shift).astype(jnp.bfloat16)
        along = jnp.dot(normed, fw_ref[...], preferred_element_type=jnp.float32).astype(
            jnp.bfloat16
        )
        total = jnp.dot(fh_ref[...], along, preferred_element_type=jnp.float32)
        plus, minus = split_rows(total, 1)
        for place, pair in ((0, plus), (mid, minus)):
            for side in range(2):
                out_ref[n, place : place + mid, side * half : (side + 1) * half] = pair[
                    side
                ].astype(jnp.bfloat16)


def mix_kernel(x_ref, w1_ref, w2_ref, bias_ref, out_ref):
    width, depth, cols = x_ref.shape
    half = cols // 2
    size = width * SUB
    for g in range(depth // (2 * SUB)):
        base = g * 2 * SUB
        values = x_ref[:, base : base + 2 * SUB, :].astype(jnp.float32)
        parts = []
        for s in range(2):
            flat = values[:, s * SUB : (s + 1) * SUB, :].reshape(size, cols).astype(jnp.bfloat16)
            both = jnp.concatenate([flat[:, :half], flat[:, half:]], axis=0)
            hid = jnp.dot(w1_ref[0], both, preferred_element_type=jnp.float32)
            hid = jnp.maximum(hid + bias_ref[0], 0.0).astype(jnp.bfloat16)
            mixed = shrink(jnp.dot(w2_ref[0], hid, preferred_element_type=jnp.float32))
            parts.append(mixed.reshape(2, width, SUB, half))
        for side in range(2):
            out_ref[:, base : base + 2 * SUB, side * half : (side + 1) * half] = (
                jnp.concatenate([parts[0][side], parts[1][side]], axis=1).astype(jnp.bfloat16)
            )


def backward_kernel(x_ref, s_ref, bh_ref, swap_ref, iw_ref, out_ref):
    count, rows, cols = x_ref.shape
    mid = rows // 2
    for n in range(count):
        total = jnp.dot(bh_ref[...], s_ref[n], preferred_element_type=jnp.float32)
        plus, minus = split_rows(total, -1)
        upper = jnp.concatenate([t.astype(jnp.bfloat16) for t in plus], axis=1)
        lower = jnp.concatenate([t.astype(jnp.bfloat16) for t in minus], axis=1)
        lower = jnp.dot(swap_ref[...], lower, preferred_element_type=jnp.float32).astype(
            jnp.bfloat16
        )
        for place, part in ((0, upper), (mid, lower)):
            filtered = jnp.dot(part, iw_ref[...], preferred_element_type=jnp.float32)
            out_ref[n, place : place + mid, :] = (
                x_ref[n, place : place + mid, :].astype(jnp.float32) + filtered
            ).astype(jnp.bfloat16)


def whole_spec(array):
    zeros = (0,) * array.ndim
    return pl.BlockSpec(array.shape, lambda i: zeros)


def per_device_local(fields, norm_gain, norm_shift, first_weight, second_weight, first_bias):
    local_ch, rows, cols = fields.shape
    half = cols // 2
    width = first_weight.shape[2]
    groups = lax.axis_size("grid")
    channels = local_ch * groups
    own_blocks = local_ch // width
    values = fields.astype(jnp.float32)
    total_sum, total_sq = lax.psum(
        (jnp.sum(values, axis=0), jnp.sum(values * values, axis=0)), "grid"
    )
    mean = total_sum / channels
    rstd = lax.rsqrt(total_sq / channels - mean * mean + 1e-05)
    fwd_w, inv_w, cos_h, sin_h = tables(rows, cols)
    low, ordered, swap = half_tables(cos_h, sin_h)
    place = lax.axis_index("grid")
    take = lambda a, size, axis: lax.dynamic_slice_in_dim(a, place * size, size, axis)
    gain_own = take(norm_gain, local_ch, 0)
    shift_own = take(norm_shift, local_ch, 0)
    first_own = spread_weight(take(first_weight, own_blocks, 1))
    second_own = spread_weight(take(second_weight, own_blocks, 1))
    bias_own = take(first_bias, local_ch, 1).reshape(2, own_blocks, width)
    bias_own = jnp.repeat(
        bias_own.transpose(1, 0, 2).reshape(own_blocks, 2 * width, 1), SUB, axis=1
    )
    size = 2 * width * SUB
    per = 2 if local_ch % 2 == 0 else 1
    params = pltpu.CompilerParams(
        dimension_semantics=("arbitrary",), vmem_limit_bytes=60 * 1024 * 1024
    )
    image = jax.ShapeDtypeStruct(fields.shape, jnp.bfloat16)
    image_spec = pl.BlockSpec((per, rows, cols), lambda i: (i, 0, 0))
    smem = pl.BlockSpec(memory_space=pltpu.SMEM)
    cost = lambda flops: pl.CostEstimate(
        flops=flops, bytes_accessed=4 * fields.size, transcendentals=0
    )
    modes = pl.pallas_call(
        forward_kernel,
        grid=(local_ch // per,),
        out_shape=image,
        in_specs=[
            image_spec,
            whole_spec(mean),
            whole_spec(rstd),
            smem,
            smem,
            whole_spec(fwd_w),
            whole_spec(low),
        ],
        out_specs=image_spec,
        compiler_params=params,
        cost_estimate=cost(2 * fields.size * (rows + cols)),
        name="forward",
    )(fields, mean, rstd, gain_own, shift_own, fwd_w, low)
    depth = 4 * SUB
    mode_spec = pl.BlockSpec((width, depth, cols), lambda b, i: (b, i, 0))
    weight_spec = pl.BlockSpec((1, size, size), lambda b, i: (b, 0, 0))
    mixed = pl.pallas_call(
        mix_kernel,
        grid=(own_blocks, rows // depth),
        out_shape=image,
        in_specs=[
            mode_spec,
            weight_spec,
            weight_spec,
            pl.BlockSpec((1, size, 1), lambda b, i: (b, 0, 0)),
        ],
        out_specs=mode_spec,
        compiler_params=pltpu.CompilerParams(
            dimension_semantics=("arbitrary", "arbitrary"), vmem_limit_bytes=60 * 1024 * 1024
        ),
        cost_estimate=cost(2 * fields.size * size),
        name="mix",
    )(modes, first_own, second_own, bias_own)
    return pl.pallas_call(
        backward_kernel,
        grid=(local_ch // per,),
        out_shape=image,
        in_specs=[
            image_spec,
            image_spec,
            whole_spec(ordered),
            whole_spec(swap),
            whole_spec(inv_w),
        ],
        out_specs=image_spec,
        compiler_params=params,
        cost_estimate=cost(2 * fields.size * (rows + cols)),
        name="backward",
    )(fields, mixed, ordered, swap, inv_w)


def per_device_any(fields, norm_gain, norm_shift, first_weight, second_weight, first_bias):
    local_ch, rows, cols = fields.shape
    whole_blocks = local_ch % first_weight.shape[2] == 0
    tiled = rows % 64 == 0 and cols % 256 == 0 and rows * cols <= 512 * 1024
    chosen = per_device_local if whole_blocks and tiled else per_device
    return chosen(fields, norm_gain, norm_shift, first_weight, second_weight, first_bias)


def solution(mesh):
    return jax.shard_map(
        per_device_any,
        mesh=mesh,
        in_specs=(P(("batch", "grid"), None, None), P(), P(), P(), P(), P()),
        out_specs=P(("batch", "grid"), None, None),
        check_vma=False,
    )
```

```python
import functools
import math

import jax
import jax.numpy as jnp
import numpy as np
from jax import lax
from jax.experimental import pallas as pl
from jax.experimental.pallas import tpu as pltpu
from jax.sharding import PartitionSpec as P


def tables(rows, cols):
    half = cols // 2
    col_index = jnp.arange(cols, dtype=jnp.int32)
    mode_index = jnp.arange(half, dtype=jnp.int32)
    angle_w = (col_index[:, None] * mode_index[None, :] % cols).astype(jnp.float32) * (
        2.0 * math.pi / cols
    )
    scale_w = 1.0 / math.sqrt(cols)
    fwd_w = jnp.concatenate(
        [jnp.cos(angle_w) * scale_w, -jnp.sin(angle_w) * scale_w], axis=1
    ).astype(jnp.bfloat16)
    weight_k = jnp.where(mode_index == 0, 1.0, 2.0).astype(jnp.float32)
    inv_w = jnp.concatenate(
        [
            (jnp.cos(angle_w) * weight_k[None, :] * scale_w).T,
            (-jnp.sin(angle_w) * weight_k[None, :] * scale_w).T,
        ],
        axis=0,
    ).astype(jnp.bfloat16)
    row_index = jnp.arange(rows, dtype=jnp.int32)
    angle_h = (row_index[:, None] * row_index[None, :] % rows).astype(jnp.float32) * (
        2.0 * math.pi / rows
    )
    scale_h = 1.0 / math.sqrt(rows)
    cos_h = (jnp.cos(angle_h) * scale_h).astype(jnp.bfloat16)
    sin_h = (jnp.sin(angle_h) * scale_h).astype(jnp.bfloat16)
    return (fwd_w, inv_w, cos_h, sin_h)


def mult(form, left, right):
    return jnp.einsum(form, left, right, preferred_element_type=jnp.float32)


def shrink(values):
    return jnp.maximum(values - 0.01, 0.0) + jnp.minimum(values + 0.01, 0.0)


def mix_modes(real_part, imag_part, first_weight, second_weight, first_bias):
    blocks = first_weight.shape[1]
    width = first_weight.shape[2]
    shape = real_part.shape
    real_blk = real_part.reshape(blocks, width, -1)
    imag_blk = imag_part.reshape(blocks, width, -1)
    bias_blk = first_bias.reshape(2, blocks, width, 1)
    hid_re = jax.nn.relu(
        mult("bio,bim->bom", first_weight[0], real_blk)
        - mult("bio,bim->bom", first_weight[1], imag_blk)
        + bias_blk[0]
    ).astype(jnp.bfloat16)
    hid_im = jax.nn.relu(
        mult("bio,bim->bom", first_weight[0], imag_blk)
        + mult("bio,bim->bom", first_weight[1], real_blk)
        + bias_blk[1]
    ).astype(jnp.bfloat16)
    out_re = mult("bio,bim->bom", second_weight[0], hid_re) - mult(
        "bio,bim->bom", second_weight[1], hid_im
    )
    out_im = mult("bio,bim->bom", second_weight[0], hid_im) + mult(
        "bio,bim->bom", second_weight[1], hid_re
    )
    return (
        shrink(out_re).astype(jnp.bfloat16).reshape(shape),
        shrink(out_im).astype(jnp.bfloat16).reshape(shape),
    )


def per_device(fields, norm_gain, norm_shift, first_weight, second_weight, first_bias):
    local_ch, rows, cols = fields.shape
    half = cols // 2
    groups = lax.axis_size("grid")
    channels = local_ch * groups
    fwd_w, inv_w, cos_h, sin_h = tables(rows, cols)
    values = fields.astype(jnp.float32)
    start = lax.axis_index("grid") * local_ch
    gain_own = lax.dynamic_slice_in_dim(norm_gain, start, local_ch)
    shift_own = lax.dynamic_slice_in_dim(norm_shift, start, local_ch)
    total_sum, total_sq = lax.psum(
        (jnp.sum(values, axis=0), jnp.sum(values * values, axis=0)), "grid"
    )
    mean = total_sum / channels
    var = total_sq / channels - mean * mean
    normed = (
        (values - mean) * lax.rsqrt(var + 1e-05) * gain_own[:, None, None]
        + shift_own[:, None, None]
    ).astype(jnp.bfloat16)
    along_w = (
        mult("chw,wk->chk", normed, fwd_w).astype(jnp.bfloat16).reshape(local_ch, rows, 2, half)
    )
    first_p = mult("kh,chpq->ckpq", cos_h, along_w)
    first_q = mult("kh,chpq->ckpq", sin_h, along_w)
    modes = jnp.stack(
        [
            (first_p[:, :, 0] + first_q[:, :, 1]).astype(jnp.bfloat16),
            (first_p[:, :, 1] - first_q[:, :, 0]).astype(jnp.bfloat16),
        ],
        axis=2,
    )
    spread = lax.all_to_all(modes, "grid", split_axis=1, concat_axis=0, tiled=True)
    shr_re, shr_im = mix_modes(
        spread[:, :, 0], spread[:, :, 1], first_weight, second_weight, first_bias
    )
    gathered = lax.all_to_all(
        jnp.stack([shr_re, shr_im], axis=2), "grid", split_axis=0, concat_axis=1, tiled=True
    )
    back_p = mult("kh,ckpq->chpq", cos_h, gathered)
    back_q = mult("kh,ckpq->chpq", sin_h, gathered)
    back_re = (back_p[:, :, 0] - back_q[:, :, 1]).astype(jnp.bfloat16)
    back_im = (back_p[:, :, 1] + back_q[:, :, 0]).astype(jnp.bfloat16)
    backed = jnp.concatenate([back_re, back_im], axis=2)
    filtered = mult("chk,kw->chw", backed, inv_w)
    return (values + filtered).astype(jnp.bfloat16)

SUB = 8


def constant_tables(rows, cols):
    half, mid = cols // 2, rows // 2
    wave = lambda f, left, right, period: f(
        (left[:, None] * right[None, :] % period).astype(np.float32)
        * np.float32(2.0 * math.pi / period)
    ) * np.float32(1.0 / math.sqrt(period))
    col, mode = np.arange(cols), np.arange(half)
    fwd_w = np.concatenate(
        [wave(np.cos, col, mode, cols), -wave(np.sin, col, mode, cols)], axis=1
    )
    weight_k = np.where(mode == 0, 1.0, 2.0).astype(np.float32)[:, None]
    inv_w = np.concatenate(
        [
            wave(np.cos, mode, col, cols) * weight_k,
            -wave(np.sin, mode, col, cols) * weight_k,
        ],
        axis=0,
    )
    row = np.arange(rows)
    cos_h, sin_h = wave(np.cos, row, row, rows), wave(np.sin, row, row, rows)
    low = np.concatenate([cos_h[: mid + 1], sin_h[1:mid]], axis=0)
    order = np.concatenate([row[: mid + 1], row[mid + 1 :][::-1]])
    swap = np.zeros((mid, mid), np.float32)
    swap[row[:mid], (mid - row[:mid]) % mid] = 1.0
    return tuple(t.astype(jnp.bfloat16) for t in (fwd_w, inv_w, low, low[:, order], swap))


def pair_weight(weight):
    real, imag = weight[0], weight[1]
    return jnp.concatenate(
        [jnp.concatenate([real, imag], axis=2), jnp.concatenate([-imag, real], axis=2)], axis=1
    )


def spread_weight(weight):
    size = weight.shape[0]
    rows = lax.broadcasted_iota(jnp.int32, (size * SUB, size), 0)
    cols = lax.broadcasted_iota(jnp.int32, (size * SUB, size), 1)
    repeat = jnp.where((rows >= cols * SUB) & (rows < cols * SUB + SUB), 1.0, 0.0).astype(
        jnp.bfloat16
    )
    last = (((1,), (1,)), ((), ()))
    tall = lax.dot_general(repeat, weight, last, preferred_element_type=jnp.float32)
    full = lax.dot_general(
        tall.astype(jnp.bfloat16), repeat, last, preferred_element_type=jnp.float32
    )
    left = lax.broadcasted_iota(jnp.int32, full.shape, 0)
    right = lax.broadcasted_iota(jnp.int32, full.shape, 1)
    return jnp.where(((left ^ right) & (SUB - 1)) == 0, full, 0.0).astype(jnp.bfloat16)


def stats_kernel(n, channels, sum_ref, sq_ref, out_ref, near, part, far, s1, r1, s2, r2, s3, r3, s4, r4):
    me = lax.axis_index("grid")
    chips = n // 2
    core, chip = lax.rem(me, 2), lax.div(me, 2)
    other = 1 - core
    sibling = chip * 2 + other
    rows = sum_ref.shape[0]
    half, piece = rows // 2, rows // n

    def ahead(j):
        return lax.rem(chip + j, chips)

    def span(c, k):
        return pl.ds(pl.multiple_of(c * half + k * piece, 8), piece)

    def send(source, target, send_sem, recv_sem, device):
        copy = pltpu.make_async_remote_copy(
            src_ref=source,
            dst_ref=target,
            send_sem=send_sem,
            recv_sem=recv_sem,
            device_id={"grid": device},
            device_id_type=pl.DeviceIdType.MESH,
        )
        copy.start()
        return copy

    barrier = pltpu.get_barrier_semaphore()
    for device in [sibling] + [ahead(j) * 2 + core for j in range(1, chips)]:
        pl.semaphore_signal(
            barrier, inc=1, device_id={"grid": device}, device_id_type=pl.DeviceIdType.MESH
        )
    pl.semaphore_wait(barrier, chips)

    theirs = pl.ds(pl.multiple_of(other * half, 8), half)
    first = [
        send(ref.at[theirs], near.at[i], s1.at[i], r1.at[i], sibling)
        for i, ref in enumerate((sum_ref, sq_ref))
    ]
    for copy in first:
        copy.wait_recv()
    second = []
    for j in range(1, chips + 1):
        k = ahead(j)
        local = pl.ds(pl.multiple_of(k * piece, 8), piece)
        for i, ref in enumerate((sum_ref, sq_ref)):
            part[j - 1, i] = ref[span(core, k)] + near[i, local]
    for j in range(1, chips):
        second.append(
            send(part.at[j - 1], far.at[j - 1], s2.at[j - 1], r2.at[j - 1], ahead(j) * 2 + core)
        )
    total_sum, total_sq = part[chips - 1, 0], part[chips - 1, 1]
    for j in range(1, chips):
        second[j - 1].wait_recv()
        total_sum = total_sum + far[j - 1, 0]
        total_sq = total_sq + far[j - 1, 1]
    mean = total_sum * (1.0 / channels)
    mine = span(core, chip)
    out_ref[0, mine] = mean
    out_ref[1, mine] = lax.rsqrt(total_sq * (1.0 / channels) - mean * mean + 1e-05)
    block = out_ref.at[:, mine]
    third = [
        send(block, block, s3.at[j - 1], r3.at[j - 1], ahead(j) * 2 + core)
        for j in range(1, chips)
    ]
    fourth = [send(block, block, s4.at[0], r4.at[0], sibling)]
    for j in range(1, chips):
        third[j - 1].wait_recv()
        block = out_ref.at[:, span(core, ahead(chips - j))]
        fourth.append(send(block, block, s4.at[j], r4.at[j], sibling))
    for copy in fourth:
        copy.wait_recv()
    for copy in first + second + third + fourth:
        copy.wait_send()


def shared_stats(total_sum, total_sq, n, channels):
    rows, cols = total_sum.shape
    chips = n // 2
    vmem = pl.BlockSpec(memory_space=pltpu.VMEM)
    counts = (2, chips - 1, chips - 1, chips)
    return pl.pallas_call(
        functools.partial(stats_kernel, n, channels),
        out_shape=jax.ShapeDtypeStruct((2, rows, cols), jnp.float32),
        in_specs=[vmem, vmem],
        out_specs=vmem,
        scratch_shapes=[
            pltpu.VMEM((2, rows // 2, cols), jnp.float32),
            pltpu.VMEM((chips, 2, rows // n, cols), jnp.float32),
            pltpu.VMEM((chips - 1, 2, rows // n, cols), jnp.float32),
        ]
        + [pltpu.SemaphoreType.DMA((c,)) for c in counts for _ in range(2)],
        compiler_params=pltpu.CompilerParams(
            collective_id=0, has_side_effects=True, vmem_limit_bytes=32 * 1024 * 1024
        ),
        name="stats",
    )(total_sum, total_sq)


def split_rows(total, sign):
    mid, half = total.shape[0] // 2, total.shape[1] // 2
    p_re, p_im = total[:mid, :half], total[:mid, half:]
    q_re, q_im = total[mid:, :half], total[mid:, half:]
    edge = lax.broadcasted_iota(jnp.int32, (mid, half), 0) == 0
    t_re = jnp.where(edge, 0.0, q_re)
    t_im = jnp.where(edge, 0.0, q_im)
    if sign < 0:
        t_re, t_im = -t_re, -t_im
    plus = (p_re + t_im, p_im - t_re)
    minus = (
        jnp.where(edge, q_re, p_re - t_im),
        jnp.where(edge, q_im, p_im + t_re),
    )
    return plus, minus


def forward_kernel(x_ref, stats_ref, gain_ref, shift_ref, fw_ref, fh_ref, out_ref):
    count, rows, cols = x_ref.shape
    mid, half = rows // 2, cols // 2
    step = pl.program_id(0)
    for n in range(count):
        gain = gain_ref[step * count + n]
        shift = shift_ref[step * count + n]
        values = x_ref[n].astype(jnp.float32)
        normed = ((values - stats_ref[0]) * stats_ref[1] * gain + shift).astype(jnp.bfloat16)
        along = jnp.dot(normed, fw_ref[...], preferred_element_type=jnp.float32).astype(
            jnp.bfloat16
        )
        total = jnp.dot(fh_ref[...], along, preferred_element_type=jnp.float32)
        plus, minus = split_rows(total, 1)
        for place, pair in ((0, plus), (mid, minus)):
            for side in range(2):
                out_ref[n, place : place + mid, side * half : (side + 1) * half] = pair[
                    side
                ].astype(jnp.bfloat16)


def mix_kernel(x_ref, first_ref, second_ref, bias_ref, out_ref, w1_ref, w2_ref):
    @pl.when(pl.program_id(1) == 0)
    def _():
        w1_ref[...] = spread_weight(first_ref[0])
        w2_ref[...] = spread_weight(second_ref[0])

    width, depth, cols = x_ref.shape
    half = cols // 2
    size = width * SUB
    for g in range(depth // (2 * SUB)):
        base = g * 2 * SUB
        values = x_ref[:, base : base + 2 * SUB, :].astype(jnp.float32)
        parts = []
        for s in range(2):
            flat = values[:, s * SUB : (s + 1) * SUB, :].reshape(size, cols).astype(jnp.bfloat16)
            both = jnp.concatenate([flat[:, :half], flat[:, half:]], axis=0)
            hid = jnp.dot(w1_ref[...], both, preferred_element_type=jnp.float32)
            hid = jnp.maximum(hid + bias_ref[0], 0.0).astype(jnp.bfloat16)
            mixed = shrink(jnp.dot(w2_ref[...], hid, preferred_element_type=jnp.float32))
            parts.append(mixed.reshape(2, width, SUB, half))
        for side in range(2):
            out_ref[:, base : base + 2 * SUB, side * half : (side + 1) * half] = (
                jnp.concatenate([parts[0][side], parts[1][side]], axis=1).astype(jnp.bfloat16)
            )


def backward_kernel(x_ref, s_ref, bh_ref, swap_ref, iw_ref, out_ref):
    count, rows, cols = x_ref.shape
    mid = rows // 2
    for n in range(count):
        total = jnp.dot(bh_ref[...], s_ref[n], preferred_element_type=jnp.float32)
        plus, minus = split_rows(total, -1)
        upper = jnp.concatenate([t.astype(jnp.bfloat16) for t in plus], axis=1)
        lower = jnp.concatenate([t.astype(jnp.bfloat16) for t in minus], axis=1)
        lower = jnp.dot(swap_ref[...], lower, preferred_element_type=jnp.float32).astype(
            jnp.bfloat16
        )
        for place, part in ((0, upper), (mid, lower)):
            filtered = jnp.dot(part, iw_ref[...], preferred_element_type=jnp.float32)
            out_ref[n, place : place + mid, :] = (
                x_ref[n, place : place + mid, :].astype(jnp.float32) + filtered
            ).astype(jnp.bfloat16)


def whole_spec(array):
    zeros = (0,) * array.ndim
    return pl.BlockSpec(array.shape, lambda i: zeros)


def per_device_local(fields, norm_gain, norm_shift, first_weight, second_weight, first_bias):
    local_ch, rows, cols = fields.shape
    half = cols // 2
    width = first_weight.shape[2]
    groups = lax.axis_size("grid")
    channels = local_ch * groups
    own_blocks = local_ch // width
    values = fields.astype(jnp.float32)
    stats = shared_stats(
        jnp.sum(values, axis=0), jnp.sum(values * values, axis=0), groups, channels
    )
    fwd_w, inv_w, low, ordered, swap = (jnp.asarray(t) for t in constant_tables(rows, cols))
    place = lax.axis_index("grid")
    take = lambda a, size, axis: lax.dynamic_slice_in_dim(a, place * size, size, axis)
    gain_own = take(norm_gain, local_ch, 0)
    shift_own = take(norm_shift, local_ch, 0)
    first_own = pair_weight(take(first_weight, own_blocks, 1))
    second_own = pair_weight(take(second_weight, own_blocks, 1))
    bias_own = take(first_bias, local_ch, 1).reshape(2, own_blocks, width)
    bias_own = jnp.repeat(
        bias_own.transpose(1, 0, 2).reshape(own_blocks, 2 * width, 1), SUB, axis=1
    )
    size = 2 * width * SUB
    per = 2 if local_ch % 2 == 0 else 1
    params = pltpu.CompilerParams(
        dimension_semantics=("arbitrary",), vmem_limit_bytes=60 * 1024 * 1024
    )
    image = jax.ShapeDtypeStruct(fields.shape, jnp.bfloat16)
    image_spec = pl.BlockSpec((per, rows, cols), lambda i: (i, 0, 0))
    smem = pl.BlockSpec(memory_space=pltpu.SMEM)
    cost = lambda flops: pl.CostEstimate(
        flops=flops, bytes_accessed=4 * fields.size, transcendentals=0
    )
    modes = pl.pallas_call(
        forward_kernel,
        grid=(local_ch // per,),
        out_shape=image,
        in_specs=[
            image_spec,
            whole_spec(stats),
            smem,
            smem,
            whole_spec(fwd_w),
            whole_spec(low),
        ],
        out_specs=image_spec,
        compiler_params=params,
        cost_estimate=cost(2 * fields.size * (rows + cols)),
        name="forward",
    )(fields, stats, gain_own, shift_own, fwd_w, low)
    depth = 4 * SUB
    mode_spec = pl.BlockSpec((width, depth, cols), lambda b, i: (b, i, 0))
    weight_spec = pl.BlockSpec((1, 2 * width, 2 * width), lambda b, i: (b, 0, 0))
    mixed = pl.pallas_call(
        mix_kernel,
        grid=(own_blocks, rows // depth),
        out_shape=image,
        in_specs=[
            mode_spec,
            weight_spec,
            weight_spec,
            pl.BlockSpec((1, size, 1), lambda b, i: (b, 0, 0)),
        ],
        out_specs=mode_spec,
        scratch_shapes=[pltpu.VMEM((size, size), jnp.bfloat16)] * 2,
        compiler_params=pltpu.CompilerParams(
            dimension_semantics=("arbitrary", "arbitrary"), vmem_limit_bytes=60 * 1024 * 1024
        ),
        cost_estimate=cost(2 * fields.size * size),
        name="mix",
    )(modes, first_own, second_own, bias_own)
    return pl.pallas_call(
        backward_kernel,
        grid=(local_ch // per,),
        out_shape=image,
        in_specs=[
            image_spec,
            image_spec,
            whole_spec(ordered),
            whole_spec(swap),
            whole_spec(inv_w),
        ],
        out_specs=image_spec,
        compiler_params=params,
        cost_estimate=cost(2 * fields.size * (rows + cols)),
        name="backward",
    )(fields, mixed, ordered, swap, inv_w)


def per_device_any(fields, norm_gain, norm_shift, first_weight, second_weight, first_bias):
    local_ch, rows, cols = fields.shape
    whole_blocks = local_ch % first_weight.shape[2] == 0
    tiled = rows % 64 == 0 and cols % 256 == 0 and rows * cols <= 512 * 1024
    groups = lax.axis_size("grid")
    tiled = tiled and groups % 2 == 0 and rows % (8 * groups) == 0
    chosen = per_device_local if whole_blocks and tiled else per_device
    return chosen(fields, norm_gain, norm_shift, first_weight, second_weight, first_bias)


def solution(mesh):
    return jax.shard_map(
        per_device_any,
        mesh=mesh,
        in_specs=(P(("batch", "grid"), None, None), P(), P(), P(), P(), P()),
        out_specs=P(("batch", "grid"), None, None),
        check_vma=False,
    )
```

```python
import functools
import math

import jax
import jax.numpy as jnp
import numpy as np
from jax import lax
from jax.experimental import pallas as pl
from jax.experimental.pallas import tpu as pltpu
from jax.sharding import PartitionSpec as P


def tables(rows, cols):
    half = cols // 2
    col_index = jnp.arange(cols, dtype=jnp.int32)
    mode_index = jnp.arange(half, dtype=jnp.int32)
    angle_w = (col_index[:, None] * mode_index[None, :] % cols).astype(jnp.float32) * (
        2.0 * math.pi / cols
    )
    scale_w = 1.0 / math.sqrt(cols)
    fwd_w = jnp.concatenate(
        [jnp.cos(angle_w) * scale_w, -jnp.sin(angle_w) * scale_w], axis=1
    ).astype(jnp.bfloat16)
    weight_k = jnp.where(mode_index == 0, 1.0, 2.0).astype(jnp.float32)
    inv_w = jnp.concatenate(
        [
            (jnp.cos(angle_w) * weight_k[None, :] * scale_w).T,
            (-jnp.sin(angle_w) * weight_k[None, :] * scale_w).T,
        ],
        axis=0,
    ).astype(jnp.bfloat16)
    row_index = jnp.arange(rows, dtype=jnp.int32)
    angle_h = (row_index[:, None] * row_index[None, :] % rows).astype(jnp.float32) * (
        2.0 * math.pi / rows
    )
    scale_h = 1.0 / math.sqrt(rows)
    cos_h = (jnp.cos(angle_h) * scale_h).astype(jnp.bfloat16)
    sin_h = (jnp.sin(angle_h) * scale_h).astype(jnp.bfloat16)
    return (fwd_w, inv_w, cos_h, sin_h)


def mult(form, left, right):
    return jnp.einsum(form, left, right, preferred_element_type=jnp.float32)


def shrink(values):
    return jnp.maximum(values - 0.01, 0.0) + jnp.minimum(values + 0.01, 0.0)


def mix_modes(real_part, imag_part, first_weight, second_weight, first_bias):
    blocks = first_weight.shape[1]
    width = first_weight.shape[2]
    shape = real_part.shape
    real_blk = real_part.reshape(blocks, width, -1)
    imag_blk = imag_part.reshape(blocks, width, -1)
    bias_blk = first_bias.reshape(2, blocks, width, 1)
    hid_re = jax.nn.relu(
        mult("bio,bim->bom", first_weight[0], real_blk)
        - mult("bio,bim->bom", first_weight[1], imag_blk)
        + bias_blk[0]
    ).astype(jnp.bfloat16)
    hid_im = jax.nn.relu(
        mult("bio,bim->bom", first_weight[0], imag_blk)
        + mult("bio,bim->bom", first_weight[1], real_blk)
        + bias_blk[1]
    ).astype(jnp.bfloat16)
    out_re = mult("bio,bim->bom", second_weight[0], hid_re) - mult(
        "bio,bim->bom", second_weight[1], hid_im
    )
    out_im = mult("bio,bim->bom", second_weight[0], hid_im) + mult(
        "bio,bim->bom", second_weight[1], hid_re
    )
    return (
        shrink(out_re).astype(jnp.bfloat16).reshape(shape),
        shrink(out_im).astype(jnp.bfloat16).reshape(shape),
    )


def per_device(fields, norm_gain, norm_shift, first_weight, second_weight, first_bias):
    local_ch, rows, cols = fields.shape
    half = cols // 2
    groups = lax.axis_size("grid")
    channels = local_ch * groups
    fwd_w, inv_w, cos_h, sin_h = tables(rows, cols)
    values = fields.astype(jnp.float32)
    start = lax.axis_index("grid") * local_ch
    gain_own = lax.dynamic_slice_in_dim(norm_gain, start, local_ch)
    shift_own = lax.dynamic_slice_in_dim(norm_shift, start, local_ch)
    total_sum, total_sq = lax.psum(
        (jnp.sum(values, axis=0), jnp.sum(values * values, axis=0)), "grid"
    )
    mean = total_sum / channels
    var = total_sq / channels - mean * mean
    normed = (
        (values - mean) * lax.rsqrt(var + 1e-05) * gain_own[:, None, None]
        + shift_own[:, None, None]
    ).astype(jnp.bfloat16)
    along_w = (
        mult("chw,wk->chk", normed, fwd_w).astype(jnp.bfloat16).reshape(local_ch, rows, 2, half)
    )
    first_p = mult("kh,chpq->ckpq", cos_h, along_w)
    first_q = mult("kh,chpq->ckpq", sin_h, along_w)
    modes = jnp.stack(
        [
            (first_p[:, :, 0] + first_q[:, :, 1]).astype(jnp.bfloat16),
            (first_p[:, :, 1] - first_q[:, :, 0]).astype(jnp.bfloat16),
        ],
        axis=2,
    )
    spread = lax.all_to_all(modes, "grid", split_axis=1, concat_axis=0, tiled=True)
    shr_re, shr_im = mix_modes(
        spread[:, :, 0], spread[:, :, 1], first_weight, second_weight, first_bias
    )
    gathered = lax.all_to_all(
        jnp.stack([shr_re, shr_im], axis=2), "grid", split_axis=0, concat_axis=1, tiled=True
    )
    back_p = mult("kh,ckpq->chpq", cos_h, gathered)
    back_q = mult("kh,ckpq->chpq", sin_h, gathered)
    back_re = (back_p[:, :, 0] - back_q[:, :, 1]).astype(jnp.bfloat16)
    back_im = (back_p[:, :, 1] + back_q[:, :, 0]).astype(jnp.bfloat16)
    backed = jnp.concatenate([back_re, back_im], axis=2)
    filtered = mult("chk,kw->chw", backed, inv_w)
    return (values + filtered).astype(jnp.bfloat16)

SUB = 8


def constant_tables(rows, cols):
    half, mid = cols // 2, rows // 2
    wave = lambda f, left, right, period: f(
        (left[:, None] * right[None, :] % period).astype(np.float32)
        * np.float32(2.0 * math.pi / period)
    ) * np.float32(1.0 / math.sqrt(period))
    col, mode = np.arange(cols), np.arange(half)
    fwd_w = np.concatenate(
        [wave(np.cos, col, mode, cols), -wave(np.sin, col, mode, cols)], axis=1
    )
    weight_k = np.where(mode == 0, 1.0, 2.0).astype(np.float32)[:, None]
    inv_w = np.concatenate(
        [
            wave(np.cos, mode, col, cols) * weight_k,
            -wave(np.sin, mode, col, cols) * weight_k,
        ],
        axis=0,
    )
    row = np.arange(rows)
    cos_h, sin_h = wave(np.cos, row, row, rows), wave(np.sin, row, row, rows)
    low = np.concatenate([cos_h[: mid + 1], sin_h[1:mid]], axis=0)
    order = np.concatenate([row[: mid + 1], row[mid + 1 :][::-1]])
    swap = np.zeros((mid, mid), np.float32)
    swap[row[:mid], (mid - row[:mid]) % mid] = 1.0
    return tuple(t.astype(jnp.bfloat16) for t in (fwd_w, inv_w, low, low[:, order], swap))


def spread_weight(weight):
    size = weight.shape[0]
    rows = lax.broadcasted_iota(jnp.int32, (size * SUB, size), 0)
    cols = lax.broadcasted_iota(jnp.int32, (size * SUB, size), 1)
    repeat = jnp.where((rows >= cols * SUB) & (rows < cols * SUB + SUB), 1.0, 0.0).astype(
        jnp.bfloat16
    )
    last = (((1,), (1,)), ((), ()))
    tall = lax.dot_general(repeat, weight, last, preferred_element_type=jnp.float32)
    full = lax.dot_general(
        tall.astype(jnp.bfloat16), repeat, last, preferred_element_type=jnp.float32
    )
    left = lax.broadcasted_iota(jnp.int32, full.shape, 0)
    right = lax.broadcasted_iota(jnp.int32, full.shape, 1)
    return jnp.where(((left ^ right) & (SUB - 1)) == 0, full, 0.0).astype(jnp.bfloat16)


def stats_kernel(n, channels, sum_ref, sq_ref, out_ref, near, part, far, s1, r1, s2, r2, s3, r3, s4, r4):
    me = lax.axis_index("grid")
    chips = n // 2
    core, chip = lax.rem(me, 2), lax.div(me, 2)
    other = 1 - core
    sibling = chip * 2 + other
    rows = sum_ref.shape[0]
    half, piece = rows // 2, rows // n

    def ahead(j):
        return lax.rem(chip + j, chips)

    def span(c, k):
        return pl.ds(pl.multiple_of(c * half + k * piece, 8), piece)

    def send(source, target, send_sem, recv_sem, device):
        copy = pltpu.make_async_remote_copy(
            src_ref=source,
            dst_ref=target,
            send_sem=send_sem,
            recv_sem=recv_sem,
            device_id={"grid": device},
            device_id_type=pl.DeviceIdType.MESH,
        )
        copy.start()
        return copy

    barrier = pltpu.get_barrier_semaphore()
    for device in [sibling] + [ahead(j) * 2 + core for j in range(1, chips)]:
        pl.semaphore_signal(
            barrier, inc=1, device_id={"grid": device}, device_id_type=pl.DeviceIdType.MESH
        )
    pl.semaphore_wait(barrier, chips)

    theirs = pl.ds(pl.multiple_of(other * half, 8), half)
    first = [
        send(ref.at[theirs], near.at[i], s1.at[i], r1.at[i], sibling)
        for i, ref in enumerate((sum_ref, sq_ref))
    ]
    for copy in first:
        copy.wait_recv()
    second = []
    for j in range(1, chips + 1):
        k = ahead(j)
        local = pl.ds(pl.multiple_of(k * piece, 8), piece)
        for i, ref in enumerate((sum_ref, sq_ref)):
            part[j - 1, i] = ref[span(core, k)] + near[i, local]
    for j in range(1, chips):
        second.append(
            send(part.at[j - 1], far.at[j - 1], s2.at[j - 1], r2.at[j - 1], ahead(j) * 2 + core)
        )
    total_sum, total_sq = part[chips - 1, 0], part[chips - 1, 1]
    for j in range(1, chips):
        second[j - 1].wait_recv()
        total_sum = total_sum + far[j - 1, 0]
        total_sq = total_sq + far[j - 1, 1]
    mean = total_sum * (1.0 / channels)
    mine = span(core, chip)
    out_ref[0, mine] = mean
    out_ref[1, mine] = lax.rsqrt(total_sq * (1.0 / channels) - mean * mean + 1e-05)
    block = out_ref.at[:, mine]
    third = [
        send(block, block, s3.at[j - 1], r3.at[j - 1], ahead(j) * 2 + core)
        for j in range(1, chips)
    ]
    fourth = [send(block, block, s4.at[0], r4.at[0], sibling)]
    for j in range(1, chips):
        third[j - 1].wait_recv()
        block = out_ref.at[:, span(core, ahead(chips - j))]
        fourth.append(send(block, block, s4.at[j], r4.at[j], sibling))
    for copy in fourth:
        copy.wait_recv()
    for copy in first + second + third + fourth:
        copy.wait_send()


def shared_stats(total_sum, total_sq, n, channels):
    rows, cols = total_sum.shape
    chips = n // 2
    vmem = pl.BlockSpec(memory_space=pltpu.VMEM)
    counts = (2, chips - 1, chips - 1, chips)
    return pl.pallas_call(
        functools.partial(stats_kernel, n, channels),
        out_shape=jax.ShapeDtypeStruct((2, rows, cols), jnp.float32),
        in_specs=[vmem, vmem],
        out_specs=vmem,
        scratch_shapes=[
            pltpu.VMEM((2, rows // 2, cols), jnp.float32),
            pltpu.VMEM((chips, 2, rows // n, cols), jnp.float32),
            pltpu.VMEM((chips - 1, 2, rows // n, cols), jnp.float32),
        ]
        + [pltpu.SemaphoreType.DMA((c,)) for c in counts for _ in range(2)],
        compiler_params=pltpu.CompilerParams(
            collective_id=0, has_side_effects=True, vmem_limit_bytes=32 * 1024 * 1024
        ),
        name="stats",
    )(total_sum, total_sq)


def split_rows(total, sign):
    mid, half = total.shape[0] // 2, total.shape[1] // 2
    p_re, p_im = total[:mid, :half], total[:mid, half:]
    q_re, q_im = total[mid:, :half], total[mid:, half:]
    edge = lax.broadcasted_iota(jnp.int32, (mid, half), 0) == 0
    t_re = jnp.where(edge, 0.0, q_re)
    t_im = jnp.where(edge, 0.0, q_im)
    if sign < 0:
        t_re, t_im = -t_re, -t_im
    plus = (p_re + t_im, p_im - t_re)
    minus = (
        jnp.where(edge, q_re, p_re - t_im),
        jnp.where(edge, q_im, p_im + t_re),
    )
    return plus, minus


def forward_kernel(x_ref, stats_ref, gain_ref, shift_ref, fw_ref, fh_ref, out_ref):
    count, rows, cols = x_ref.shape
    mid, half = rows // 2, cols // 2
    start = (lax.axis_index("grid") * pl.num_programs(0) + pl.program_id(0)) * count
    for n in range(count):
        gain = gain_ref[start + n]
        shift = shift_ref[start + n]
        values = x_ref[n].astype(jnp.float32)
        normed = ((values - stats_ref[0]) * stats_ref[1] * gain + shift).astype(jnp.bfloat16)
        along = jnp.dot(normed, fw_ref[...], preferred_element_type=jnp.float32).astype(
            jnp.bfloat16
        )
        total = jnp.dot(fh_ref[...], along, preferred_element_type=jnp.float32)
        plus, minus = split_rows(total, 1)
        for place, pair in ((0, plus), (mid, minus)):
            for side in range(2):
                out_ref[n, place : place + mid, side * half : (side + 1) * half] = pair[
                    side
                ].astype(jnp.bfloat16)


def mix_kernel(x_ref, first_ref, second_ref, bias_ref, out_ref, w1_ref, w2_ref, b1_ref):
    @pl.when(pl.program_id(1) == 0)
    def _():
        block = lax.axis_index("grid") * pl.num_programs(0) + pl.program_id(0)
        width = first_ref.shape[2]
        size = width * SUB
        for source, target in ((first_ref, w1_ref), (second_ref, w2_ref)):
            real = spread_weight(source[0, block])
            imag = spread_weight(source[1, block])
            target[:size, :size] = real
            target[:size, size:] = -imag
            target[size:, :size] = imag
            target[size:, size:] = real
        shape = (size, bias_ref.shape[1])
        first = (lax.broadcasted_iota(jnp.int32, shape, 1) - block * width) * SUB
        offset = lax.broadcasted_iota(jnp.int32, shape, 0) - first
        own = (offset >= 0) & (offset < SUB)
        for side in range(2):
            picked = jnp.where(own, bias_ref[side : side + 1, :], 0.0)
            b1_ref[side * size : (side + 1) * size, :] = jnp.sum(picked, axis=1, keepdims=True)

    width, depth, cols = x_ref.shape
    half = cols // 2
    size = width * SUB
    for g in range(depth // (2 * SUB)):
        base = g * 2 * SUB
        values = x_ref[:, base : base + 2 * SUB, :].astype(jnp.float32)
        parts = []
        for s in range(2):
            flat = values[:, s * SUB : (s + 1) * SUB, :].reshape(size, cols).astype(jnp.bfloat16)
            both = jnp.concatenate([flat[:, :half], flat[:, half:]], axis=0)
            hid = jnp.dot(w1_ref[...], both, preferred_element_type=jnp.float32)
            hid = jnp.maximum(hid + b1_ref[...], 0.0).astype(jnp.bfloat16)
            mixed = jnp.dot(w2_ref[...], hid, preferred_element_type=jnp.float32)
            mixed = mixed - jnp.clip(mixed, -0.01, 0.01)
            parts.append(mixed.reshape(2, width, SUB, half))
        for side in range(2):
            out_ref[:, base : base + 2 * SUB, side * half : (side + 1) * half] = (
                jnp.concatenate([parts[0][side], parts[1][side]], axis=1).astype(jnp.bfloat16)
            )


def backward_kernel(x_ref, s_ref, bh_ref, swap_ref, iw_ref, out_ref):
    count, rows, cols = x_ref.shape
    mid = rows // 2
    for n in range(count):
        total = jnp.dot(bh_ref[...], s_ref[n], preferred_element_type=jnp.float32)
        plus, minus = split_rows(total, -1)
        upper = jnp.concatenate([t.astype(jnp.bfloat16) for t in plus], axis=1)
        lower = jnp.concatenate([t.astype(jnp.bfloat16) for t in minus], axis=1)
        lower = jnp.dot(swap_ref[...], lower, preferred_element_type=jnp.float32).astype(
            jnp.bfloat16
        )
        for place, part in ((0, upper), (mid, lower)):
            filtered = jnp.dot(part, iw_ref[...], preferred_element_type=jnp.float32)
            out_ref[n, place : place + mid, :] = (
                x_ref[n, place : place + mid, :].astype(jnp.float32) + filtered
            ).astype(jnp.bfloat16)


def whole_spec(array):
    zeros = (0,) * array.ndim
    return pl.BlockSpec(array.shape, lambda *_: zeros)


def per_device_local(fields, norm_gain, norm_shift, first_weight, second_weight, first_bias):
    local_ch, rows, cols = fields.shape
    half = cols // 2
    width = first_weight.shape[2]
    groups = lax.axis_size("grid")
    channels = local_ch * groups
    own_blocks = local_ch // width
    values = fields.astype(jnp.float32)
    stats = shared_stats(
        jnp.sum(values, axis=0), jnp.sum(values * values, axis=0), groups, channels
    )
    fwd_w, inv_w, low, ordered, swap = (jnp.asarray(t) for t in constant_tables(rows, cols))
    size = 2 * width * SUB
    per = 2 if local_ch % 2 == 0 else 1
    params = pltpu.CompilerParams(
        dimension_semantics=("arbitrary",), vmem_limit_bytes=60 * 1024 * 1024
    )
    image = jax.ShapeDtypeStruct(fields.shape, jnp.bfloat16)
    image_spec = pl.BlockSpec((per, rows, cols), lambda i: (i, 0, 0))
    smem = pl.BlockSpec(memory_space=pltpu.SMEM)
    cost = lambda flops: pl.CostEstimate(
        flops=flops, bytes_accessed=4 * fields.size, transcendentals=0
    )
    modes = pl.pallas_call(
        forward_kernel,
        grid=(local_ch // per,),
        out_shape=image,
        in_specs=[
            image_spec,
            whole_spec(stats),
            smem,
            smem,
            whole_spec(fwd_w),
            whole_spec(low),
        ],
        out_specs=image_spec,
        compiler_params=params,
        cost_estimate=cost(2 * fields.size * (rows + cols)),
        name="forward",
    )(fields, stats, norm_gain, norm_shift, fwd_w, low)
    depth = 4 * SUB
    mode_spec = pl.BlockSpec((width, depth, cols), lambda b, i: (b, i, 0))
    mixed = pl.pallas_call(
        mix_kernel,
        grid=(own_blocks, rows // depth),
        out_shape=image,
        in_specs=[
            mode_spec,
            whole_spec(first_weight),
            whole_spec(second_weight),
            whole_spec(first_bias),
        ],
        out_specs=mode_spec,
        scratch_shapes=[pltpu.VMEM((size, size), jnp.bfloat16)] * 2
        + [pltpu.VMEM((size, 1), jnp.float32)],
        compiler_params=pltpu.CompilerParams(
            dimension_semantics=("arbitrary", "arbitrary"), vmem_limit_bytes=60 * 1024 * 1024
        ),
        cost_estimate=cost(2 * fields.size * size),
        name="mix",
    )(modes, first_weight, second_weight, first_bias)
    return pl.pallas_call(
        backward_kernel,
        grid=(local_ch // per,),
        out_shape=image,
        in_specs=[
            image_spec,
            image_spec,
            whole_spec(ordered),
            whole_spec(swap),
            whole_spec(inv_w),
        ],
        out_specs=image_spec,
        compiler_params=params,
        cost_estimate=cost(2 * fields.size * (rows + cols)),
        name="backward",
    )(fields, mixed, ordered, swap, inv_w)


def per_device_any(fields, norm_gain, norm_shift, first_weight, second_weight, first_bias):
    local_ch, rows, cols = fields.shape
    whole_blocks = local_ch % first_weight.shape[2] == 0
    tiled = rows % 64 == 0 and cols % 256 == 0 and rows * cols <= 512 * 1024
    groups = lax.axis_size("grid")
    tiled = tiled and groups % 2 == 0 and rows % (8 * groups) == 0
    chosen = per_device_local if whole_blocks and tiled else per_device
    return chosen(fields, norm_gain, norm_shift, first_weight, second_weight, first_bias)


def solution(mesh):
    return jax.shard_map(
        per_device_any,
        mesh=mesh,
        in_specs=(P(("batch", "grid"), None, None), P(), P(), P(), P(), P()),
        out_specs=P(("batch", "grid"), None, None),
        check_vma=False,
    )
```

```python
import functools
import math

import jax
import jax.numpy as jnp
import numpy as np
from jax import lax
from jax.experimental import pallas as pl
from jax.experimental.pallas import tpu as pltpu
from jax.sharding import PartitionSpec as P


def tables(rows, cols):
    half = cols // 2
    col_index = jnp.arange(cols, dtype=jnp.int32)
    mode_index = jnp.arange(half, dtype=jnp.int32)
    angle_w = (col_index[:, None] * mode_index[None, :] % cols).astype(jnp.float32) * (
        2.0 * math.pi / cols
    )
    scale_w = 1.0 / math.sqrt(cols)
    fwd_w = jnp.concatenate(
        [jnp.cos(angle_w) * scale_w, -jnp.sin(angle_w) * scale_w], axis=1
    ).astype(jnp.bfloat16)
    weight_k = jnp.where(mode_index == 0, 1.0, 2.0).astype(jnp.float32)
    inv_w = jnp.concatenate(
        [
            (jnp.cos(angle_w) * weight_k[None, :] * scale_w).T,
            (-jnp.sin(angle_w) * weight_k[None, :] * scale_w).T,
        ],
        axis=0,
    ).astype(jnp.bfloat16)
    row_index = jnp.arange(rows, dtype=jnp.int32)
    angle_h = (row_index[:, None] * row_index[None, :] % rows).astype(jnp.float32) * (
        2.0 * math.pi / rows
    )
    scale_h = 1.0 / math.sqrt(rows)
    cos_h = (jnp.cos(angle_h) * scale_h).astype(jnp.bfloat16)
    sin_h = (jnp.sin(angle_h) * scale_h).astype(jnp.bfloat16)
    return (fwd_w, inv_w, cos_h, sin_h)


def mult(form, left, right):
    return jnp.einsum(form, left, right, preferred_element_type=jnp.float32)


def shrink(values):
    return jnp.maximum(values - 0.01, 0.0) + jnp.minimum(values + 0.01, 0.0)


def mix_modes(real_part, imag_part, first_weight, second_weight, first_bias):
    blocks = first_weight.shape[1]
    width = first_weight.shape[2]
    shape = real_part.shape
    real_blk = real_part.reshape(blocks, width, -1)
    imag_blk = imag_part.reshape(blocks, width, -1)
    bias_blk = first_bias.reshape(2, blocks, width, 1)
    hid_re = jax.nn.relu(
        mult("bio,bim->bom", first_weight[0], real_blk)
        - mult("bio,bim->bom", first_weight[1], imag_blk)
        + bias_blk[0]
    ).astype(jnp.bfloat16)
    hid_im = jax.nn.relu(
        mult("bio,bim->bom", first_weight[0], imag_blk)
        + mult("bio,bim->bom", first_weight[1], real_blk)
        + bias_blk[1]
    ).astype(jnp.bfloat16)
    out_re = mult("bio,bim->bom", second_weight[0], hid_re) - mult(
        "bio,bim->bom", second_weight[1], hid_im
    )
    out_im = mult("bio,bim->bom", second_weight[0], hid_im) + mult(
        "bio,bim->bom", second_weight[1], hid_re
    )
    return (
        shrink(out_re).astype(jnp.bfloat16).reshape(shape),
        shrink(out_im).astype(jnp.bfloat16).reshape(shape),
    )


def per_device(fields, norm_gain, norm_shift, first_weight, second_weight, first_bias):
    local_ch, rows, cols = fields.shape
    half = cols // 2
    groups = lax.axis_size("grid")
    channels = local_ch * groups
    fwd_w, inv_w, cos_h, sin_h = tables(rows, cols)
    values = fields.astype(jnp.float32)
    start = lax.axis_index("grid") * local_ch
    gain_own = lax.dynamic_slice_in_dim(norm_gain, start, local_ch)
    shift_own = lax.dynamic_slice_in_dim(norm_shift, start, local_ch)
    total_sum, total_sq = lax.psum(
        (jnp.sum(values, axis=0), jnp.sum(values * values, axis=0)), "grid"
    )
    mean = total_sum / channels
    var = total_sq / channels - mean * mean
    normed = (
        (values - mean) * lax.rsqrt(var + 1e-05) * gain_own[:, None, None]
        + shift_own[:, None, None]
    ).astype(jnp.bfloat16)
    along_w = (
        mult("chw,wk->chk", normed, fwd_w).astype(jnp.bfloat16).reshape(local_ch, rows, 2, half)
    )
    first_p = mult("kh,chpq->ckpq", cos_h, along_w)
    first_q = mult("kh,chpq->ckpq", sin_h, along_w)
    modes = jnp.stack(
        [
            (first_p[:, :, 0] + first_q[:, :, 1]).astype(jnp.bfloat16),
            (first_p[:, :, 1] - first_q[:, :, 0]).astype(jnp.bfloat16),
        ],
        axis=2,
    )
    spread = lax.all_to_all(modes, "grid", split_axis=1, concat_axis=0, tiled=True)
    shr_re, shr_im = mix_modes(
        spread[:, :, 0], spread[:, :, 1], first_weight, second_weight, first_bias
    )
    gathered = lax.all_to_all(
        jnp.stack([shr_re, shr_im], axis=2), "grid", split_axis=0, concat_axis=1, tiled=True
    )
    back_p = mult("kh,ckpq->chpq", cos_h, gathered)
    back_q = mult("kh,ckpq->chpq", sin_h, gathered)
    back_re = (back_p[:, :, 0] - back_q[:, :, 1]).astype(jnp.bfloat16)
    back_im = (back_p[:, :, 1] + back_q[:, :, 0]).astype(jnp.bfloat16)
    backed = jnp.concatenate([back_re, back_im], axis=2)
    filtered = mult("chk,kw->chw", backed, inv_w)
    return (values + filtered).astype(jnp.bfloat16)

SUB = 8


def constant_tables(rows, cols):
    half, mid = cols // 2, rows // 2
    wave = lambda f, left, right, period: f(
        (left[:, None] * right[None, :] % period).astype(np.float32)
        * np.float32(2.0 * math.pi / period)
    ) * np.float32(1.0 / math.sqrt(period))
    col, mode = np.arange(cols), np.arange(half)
    fwd_w = np.concatenate(
        [wave(np.cos, col, mode, cols), -wave(np.sin, col, mode, cols)], axis=1
    )
    weight_k = np.where(mode == 0, 1.0, 2.0).astype(np.float32)[:, None]
    inv_w = np.concatenate(
        [
            wave(np.cos, mode, col, cols) * weight_k,
            -wave(np.sin, mode, col, cols) * weight_k,
        ],
        axis=0,
    )
    row = np.arange(rows)
    cos_h, sin_h = wave(np.cos, row, row, rows), wave(np.sin, row, row, rows)
    low = np.concatenate([cos_h[: mid + 1], sin_h[1:mid]], axis=0)
    order = np.concatenate([row[: mid + 1], row[mid + 1 :][::-1]])
    swap = np.zeros((mid, mid), np.float32)
    swap[row[:mid], (mid - row[:mid]) % mid] = 1.0
    return tuple(t.astype(jnp.bfloat16) for t in (fwd_w, inv_w, low, low[:, order], swap))


def spread_weight(weight):
    size = weight.shape[0]
    rows = lax.broadcasted_iota(jnp.int32, (size * SUB, size), 0)
    cols = lax.broadcasted_iota(jnp.int32, (size * SUB, size), 1)
    repeat = jnp.where((rows >= cols * SUB) & (rows < cols * SUB + SUB), 1.0, 0.0).astype(
        jnp.bfloat16
    )
    last = (((1,), (1,)), ((), ()))
    tall = lax.dot_general(repeat, weight, last, preferred_element_type=jnp.float32)
    full = lax.dot_general(
        tall.astype(jnp.bfloat16), repeat, last, preferred_element_type=jnp.float32
    )
    left = lax.broadcasted_iota(jnp.int32, full.shape, 0)
    right = lax.broadcasted_iota(jnp.int32, full.shape, 1)
    return jnp.where(((left ^ right) & (SUB - 1)) == 0, full, 0.0).astype(jnp.bfloat16)


def stats_kernel(n, channels, sum_ref, sq_ref, out_ref, near, part, far, s1, r1, s2, r2, s3, r3, s4, r4):
    me = lax.axis_index("grid")
    chips = n // 2
    core, chip = lax.rem(me, 2), lax.div(me, 2)
    other = 1 - core
    sibling = chip * 2 + other
    rows = sum_ref.shape[0]
    half, piece = rows // 2, rows // n

    def ahead(j):
        return lax.rem(chip + j, chips)

    def span(c, k):
        return pl.ds(pl.multiple_of(c * half + k * piece, 8), piece)

    def send(source, target, send_sem, recv_sem, device):
        copy = pltpu.make_async_remote_copy(
            src_ref=source,
            dst_ref=target,
            send_sem=send_sem,
            recv_sem=recv_sem,
            device_id={"grid": device},
            device_id_type=pl.DeviceIdType.MESH,
        )
        copy.start()
        return copy

    barrier = pltpu.get_barrier_semaphore()
    for device in [sibling] + [ahead(j) * 2 + core for j in range(1, chips)]:
        pl.semaphore_signal(
            barrier, inc=1, device_id={"grid": device}, device_id_type=pl.DeviceIdType.MESH
        )
    pl.semaphore_wait(barrier, chips)

    theirs = pl.ds(pl.multiple_of(other * half, 8), half)
    first = [
        send(ref.at[theirs], near.at[i], s1.at[i], r1.at[i], sibling)
        for i, ref in enumerate((sum_ref, sq_ref))
    ]
    for copy in first:
        copy.wait_recv()
    second = []
    for j in range(1, chips + 1):
        k = ahead(j)
        local = pl.ds(pl.multiple_of(k * piece, 8), piece)
        for i, ref in enumerate((sum_ref, sq_ref)):
            part[j - 1, i] = ref[span(core, k)] + near[i, local]
    for j in range(1, chips):
        second.append(
            send(part.at[j - 1], far.at[j - 1], s2.at[j - 1], r2.at[j - 1], ahead(j) * 2 + core)
        )
    total_sum, total_sq = part[chips - 1, 0], part[chips - 1, 1]
    for j in range(1, chips):
        second[j - 1].wait_recv()
        total_sum = total_sum + far[j - 1, 0]
        total_sq = total_sq + far[j - 1, 1]
    mean = total_sum * (1.0 / channels)
    mine = span(core, chip)
    out_ref[0, mine] = mean
    out_ref[1, mine] = lax.rsqrt(total_sq * (1.0 / channels) - mean * mean + 1e-05)
    block = out_ref.at[:, mine]
    third = [
        send(block, block, s3.at[j - 1], r3.at[j - 1], ahead(j) * 2 + core)
        for j in range(1, chips)
    ]
    fourth = [send(block, block, s4.at[0], r4.at[0], sibling)]
    for j in range(1, chips):
        third[j - 1].wait_recv()
        block = out_ref.at[:, span(core, ahead(chips - j))]
        fourth.append(send(block, block, s4.at[j], r4.at[j], sibling))
    for copy in fourth:
        copy.wait_recv()
    for copy in first + second + third + fourth:
        copy.wait_send()


def shared_stats(total_sum, total_sq, n, channels):
    rows, cols = total_sum.shape
    chips = n // 2
    vmem = pl.BlockSpec(memory_space=pltpu.VMEM)
    counts = (2, chips - 1, chips - 1, chips)
    return pl.pallas_call(
        functools.partial(stats_kernel, n, channels),
        out_shape=jax.ShapeDtypeStruct((2, rows, cols), jnp.float32),
        in_specs=[vmem, vmem],
        out_specs=vmem,
        scratch_shapes=[
            pltpu.VMEM((2, rows // 2, cols), jnp.float32),
            pltpu.VMEM((chips, 2, rows // n, cols), jnp.float32),
            pltpu.VMEM((chips - 1, 2, rows // n, cols), jnp.float32),
        ]
        + [pltpu.SemaphoreType.DMA((c,)) for c in counts for _ in range(2)],
        compiler_params=pltpu.CompilerParams(
            collective_id=0, has_side_effects=True, vmem_limit_bytes=32 * 1024 * 1024
        ),
        name="stats",
    )(total_sum, total_sq)


def split_rows(total, sign):
    mid, half = total.shape[0] // 2, total.shape[1] // 2
    p_re, p_im = total[:mid, :half], total[:mid, half:]
    q_re, q_im = total[mid:, :half], total[mid:, half:]
    edge = lax.broadcasted_iota(jnp.int32, (mid, half), 0) == 0
    t_re = jnp.where(edge, 0.0, q_re)
    t_im = jnp.where(edge, 0.0, q_im)
    if sign < 0:
        t_re, t_im = -t_re, -t_im
    plus = (p_re + t_im, p_im - t_re)
    minus = (
        jnp.where(edge, q_re, p_re - t_im),
        jnp.where(edge, q_im, p_im + t_re),
    )
    return plus, minus


def forward_kernel(x_ref, stats_ref, gain_ref, shift_ref, fw_ref, fh_ref, out_ref):
    count, rows, cols = x_ref.shape
    mid, half = rows // 2, cols // 2
    start = (lax.axis_index("grid") * pl.num_programs(0) + pl.program_id(0)) * count
    for n in range(count):
        gain = gain_ref[start + n]
        shift = shift_ref[start + n]
        values = x_ref[n].astype(jnp.float32)
        normed = ((values - stats_ref[0]) * stats_ref[1] * gain + shift).astype(jnp.bfloat16)
        along = jnp.dot(normed, fw_ref[...], preferred_element_type=jnp.float32).astype(
            jnp.bfloat16
        )
        total = jnp.dot(fh_ref[...], along, preferred_element_type=jnp.float32)
        plus, minus = split_rows(total, 1)
        for place, pair in ((0, plus), (mid, minus)):
            for side in range(2):
                out_ref[n, place : place + mid, side * half : (side + 1) * half] = pair[
                    side
                ].astype(jnp.bfloat16)


def mix_kernel(x_ref, first_ref, second_ref, bias_ref, out_ref, w1_ref, w2_ref, b1_ref):
    @pl.when(pl.program_id(1) == 0)
    def _():
        block = lax.axis_index("grid") * pl.num_programs(0) + pl.program_id(0)
        width = first_ref.shape[2]
        size = width * SUB
        for source, target in ((first_ref, w1_ref), (second_ref, w2_ref)):
            real = spread_weight(source[0, block])
            imag = spread_weight(source[1, block])
            target[:size, :size] = real
            target[:size, size:] = -imag
            target[size:, :size] = imag
            target[size:, size:] = real
        shape = (size, bias_ref.shape[1])
        first = (lax.broadcasted_iota(jnp.int32, shape, 1) - block * width) * SUB
        offset = lax.broadcasted_iota(jnp.int32, shape, 0) - first
        own = (offset >= 0) & (offset < SUB)
        for side in range(2):
            picked = jnp.where(own, bias_ref[side : side + 1, :], 0.0)
            b1_ref[side * size : (side + 1) * size, :] = jnp.sum(picked, axis=1, keepdims=True)

    width, depth, cols = x_ref.shape
    half = cols // 2
    size = width * SUB
    for g in range(depth // (2 * SUB)):
        base = g * 2 * SUB
        values = x_ref[:, base : base + 2 * SUB, :].astype(jnp.float32)
        parts = []
        for s in range(2):
            flat = values[:, s * SUB : (s + 1) * SUB, :].reshape(size, cols).astype(jnp.bfloat16)
            both = jnp.concatenate([flat[:, :half], flat[:, half:]], axis=0)
            hid = jnp.dot(w1_ref[...], both, preferred_element_type=jnp.float32)
            hid = jnp.maximum(hid + b1_ref[...], 0.0).astype(jnp.bfloat16)
            mixed = jnp.dot(w2_ref[...], hid, preferred_element_type=jnp.float32)
            mixed = mixed - jnp.clip(mixed, -0.01, 0.01)
            parts.append(mixed.reshape(2, width, SUB, half))
        for side in range(2):
            out_ref[:, base : base + 2 * SUB, side * half : (side + 1) * half] = (
                jnp.concatenate([parts[0][side], parts[1][side]], axis=1).astype(jnp.bfloat16)
            )


def backward_kernel(x_ref, s_ref, bh_ref, swap_ref, iw_ref, out_ref):
    count, rows, cols = x_ref.shape
    mid = rows // 2
    for n in range(count):
        total = jnp.dot(bh_ref[...], s_ref[n], preferred_element_type=jnp.float32)
        plus, minus = split_rows(total, -1)
        upper = jnp.concatenate([t.astype(jnp.bfloat16) for t in plus], axis=1)
        lower = jnp.concatenate([t.astype(jnp.bfloat16) for t in minus], axis=1)
        lower = jnp.dot(swap_ref[...], lower, preferred_element_type=jnp.float32).astype(
            jnp.bfloat16
        )
        for place, part in ((0, upper), (mid, lower)):
            filtered = jnp.dot(part, iw_ref[...], preferred_element_type=jnp.float32)
            out_ref[n, place : place + mid, :] = (
                x_ref[n, place : place + mid, :].astype(jnp.float32) + filtered
            ).astype(jnp.bfloat16)


def whole_spec(array):
    zeros = (0,) * array.ndim
    return pl.BlockSpec(array.shape, lambda *_: zeros)


def per_device_local(fields, norm_gain, norm_shift, first_weight, second_weight, first_bias):
    local_ch, rows, cols = fields.shape
    half = cols // 2
    width = first_weight.shape[2]
    groups = lax.axis_size("grid")
    channels = local_ch * groups
    own_blocks = local_ch // width
    values = fields.astype(jnp.float32)
    stats = shared_stats(
        jnp.sum(values, axis=0), jnp.sum(values * values, axis=0), groups, channels
    )
    fwd_w, inv_w, low, ordered, swap = (jnp.asarray(t) for t in constant_tables(rows, cols))
    size = 2 * width * SUB
    per = 4 if local_ch % 4 == 0 else 1
    params = pltpu.CompilerParams(
        dimension_semantics=("arbitrary",), vmem_limit_bytes=60 * 1024 * 1024
    )
    image = jax.ShapeDtypeStruct(fields.shape, jnp.bfloat16)
    image_spec = pl.BlockSpec((per, rows, cols), lambda i: (i, 0, 0))
    smem = pl.BlockSpec(memory_space=pltpu.SMEM)
    cost = lambda flops: pl.CostEstimate(
        flops=flops, bytes_accessed=4 * fields.size, transcendentals=0
    )
    modes = pl.pallas_call(
        forward_kernel,
        grid=(local_ch // per,),
        out_shape=image,
        in_specs=[
            image_spec,
            whole_spec(stats),
            smem,
            smem,
            whole_spec(fwd_w),
            whole_spec(low),
        ],
        out_specs=image_spec,
        compiler_params=params,
        cost_estimate=cost(2 * fields.size * (rows + cols)),
        name="forward",
    )(fields, stats, norm_gain, norm_shift, fwd_w, low)
    depth = 8 * SUB
    mode_spec = pl.BlockSpec((width, depth, cols), lambda b, i: (b, i, 0))
    mixed = pl.pallas_call(
        mix_kernel,
        grid=(own_blocks, rows // depth),
        out_shape=image,
        in_specs=[
            mode_spec,
            whole_spec(first_weight),
            whole_spec(second_weight),
            whole_spec(first_bias),
        ],
        out_specs=mode_spec,
        scratch_shapes=[pltpu.VMEM((size, size), jnp.bfloat16)] * 2
        + [pltpu.VMEM((size, 1), jnp.float32)],
        compiler_params=pltpu.CompilerParams(
            dimension_semantics=("arbitrary", "arbitrary"), vmem_limit_bytes=60 * 1024 * 1024
        ),
        cost_estimate=cost(2 * fields.size * size),
        name="mix",
    )(modes, first_weight, second_weight, first_bias)
    return pl.pallas_call(
        backward_kernel,
        grid=(local_ch // per,),
        out_shape=image,
        in_specs=[
            image_spec,
            image_spec,
            whole_spec(ordered),
            whole_spec(swap),
            whole_spec(inv_w),
        ],
        out_specs=image_spec,
        compiler_params=params,
        cost_estimate=cost(2 * fields.size * (rows + cols)),
        name="backward",
    )(fields, mixed, ordered, swap, inv_w)


def per_device_any(fields, norm_gain, norm_shift, first_weight, second_weight, first_bias):
    local_ch, rows, cols = fields.shape
    whole_blocks = local_ch % first_weight.shape[2] == 0
    tiled = rows % 64 == 0 and cols % 256 == 0 and rows * cols <= 512 * 1024
    groups = lax.axis_size("grid")
    tiled = tiled and groups % 2 == 0 and rows % (8 * groups) == 0
    chosen = per_device_local if whole_blocks and tiled else per_device
    return chosen(fields, norm_gain, norm_shift, first_weight, second_weight, first_bias)


def solution(mesh):
    return jax.shard_map(
        per_device_any,
        mesh=mesh,
        in_specs=(P(("batch", "grid"), None, None), P(), P(), P(), P(), P()),
        out_specs=P(("batch", "grid"), None, None),
        check_vma=False,
    )
```
